256 devices in a mesh: head: 8 (over z_hi, core), outer: 2 (over z_lo), inner: 16 (over y, x).
Axes of the slice: x: 4, y: 4, z: 8 (z_hi: 4, z_lo: 2; z = z_hi * 2 + z_lo), core: 2. Of those that a mesh axis runs over, the one named last changes fastest.
Arguments:
- query: bfloat16 [32768, 8192], P(('outer', 'inner', 'head')), may hold values from -100 to 100
- keys: bfloat16 [32768, 1024], P(('outer', 'inner', 'head')), may hold values from -4.5 to 4.5
- values: bfloat16 [32768, 1024], P(('outer', 'inner', 'head')), may hold values from -6 to 6
- lengths: int32 [32], replicated, may hold values from 1 to 2048, 32768 in all
Outputs:
- attended: bfloat16 [32768, 8192], P(('outer', 'inner', 'head'))
The draws below stay inside these ranges and needn't reach their ends.
Inputs may be any that keep to these rules, and one draw needn't show every extreme that they name: `lengths`: they sum to 32768, and the longest is exactly 2048.
All inputs are finite; a program needn't handle non-finite values.
Results may differ from the reference program's by a relative error of at most 0.0038.
Values may be sent and summed in bfloat16 or wider, within the bound.
A program may use at most 64 MiB of HBM per device.

```python
import math
import jax
import jax.numpy as jnp
import numpy as np
from jax import lax

QUERY_HEAD_COUNT = 64
KEY_VALUE_HEADS = 8
HEAD_SIZE = 128
NEARBY_TOKENS = 1024
PACKED_TOKENS = 32768
REACH = 2
MAXDOC = 2048
NDOCS = 32


def starting_keys(key):
    sampled = jnp.clip(jax.random.normal(jax.random.fold_in(key, 30), (PACKED_TOKENS, KEY_VALUE_HEADS * HEAD_SIZE), jnp.float32), -4.5, 4.5)
    return sampled


def draw_keys(key, part):
    return starting_keys(key).astype(jnp.bfloat16)


def draw_query(key, part):
    result = jnp.clip(jax.random.normal(jax.random.fold_in(key, 40), (PACKED_TOKENS, QUERY_HEAD_COUNT * HEAD_SIZE), jnp.float32), -4.5, 4.5)
    return result.astype(jnp.bfloat16)


def block_levels(key, shape, shards, low, high):
    factor_of = 1.0
    for axis_at, parts in shards:
        steps = jax.random.uniform(jax.random.fold_in(jax.random.fold_in(key, 6), axis_at), (parts,), jnp.float32, low / len(shards), high / len(shards))
        factor_of = factor_of * jnp.repeat(jnp.exp(steps), shape[axis_at] // parts).reshape((-1,) + (1,) * (len(shape) - 1 - axis_at))
    return factor_of


def split_up(amount, total, limit, skew):
    loads = [(1 << 20) // math.isqrt(rank ** skew) + 1 for rank in range(2, amount + 1)]
    rest, given = total - limit - (amount - 1), [1] * (amount - 1)
    while rest > 0:
        candidates = [i for i in range(amount - 1) if given[i] < limit]
        pool, remaining = sum([loads[i] for i in candidates]), rest
        for i in candidates:
            addition = min(limit - given[i], max(1, remaining * loads[i] // pool), rest)
            given[i] = given[i] + addition
            rest = rest - addition
    return np.array([limit] + given)


def uneven_parts(stream_key, amount, total, most, lean):
    if amount == 2:
        one = jax.random.randint(stream_key, (), max(1, total - most), min(most, total - 1) + 1)
        return jnp.stack([one, total - one])
    sizes = jnp.asarray(split_up(amount, total, most, lean), jnp.int32)
    twos = (amount - 1) // 2
    donor, taker = sizes[1:1 + 2 * twos:2], sizes[2:2 + 2 * twos:2]
    margin = jnp.minimum(donor - 1, most - taker)
    shifted = jax.random.randint(jax.random.fold_in(stream_key, 1), (twos,), 0, 1 << 20) % (margin + 1)
    sizes = sizes.at[1:1 + 2 * twos:2].set(donor - shifted).at[2:2 + 2 * twos:2].set(taker + shifted)
    return sizes[jax.random.permutation(jax.random.fold_in(stream_key, 2), amount)]


def scatter_about(own_key, extent, deviation, reach, pieces=(), kind=jnp.bfloat16):
    level = block_levels(own_key, extent, pieces, -0.22, 0.18) if pieces else 1.0
    drawn = jax.random.normal(own_key, extent, jnp.float32) * deviation * level
    return jnp.minimum(jnp.maximum(drawn, -reach), reach).astype(kind)


def setup_inputs(seed: int = 0) -> dict:
    streams_of = jax.random.split(jax.random.key(seed), 5)
    query = draw_query(jax.random.fold_in(streams_of[4], 71), 0)
    keys = draw_keys(jax.random.fold_in(streams_of[4], 71), 0)
    values = scatter_about(streams_of[2], (PACKED_TOKENS, KEY_VALUE_HEADS * HEAD_SIZE), 1.0, 6.0, ((0, 256),))
    lengths = uneven_parts(streams_of[3], NDOCS, PACKED_TOKENS, MAXDOC, 2).astype(jnp.int32)
    return dict(query=query, keys=keys, values=values, lengths=lengths)


def doc_of(lengths, positions):
    ends = jnp.cumsum(lengths)
    return lax.optimization_barrier(jnp.sum((positions[:, None] >= ends[None, :]).astype(jnp.int32), axis=1))

def reference(query, keys, values, lengths):
    group_width = QUERY_HEAD_COUNT // KEY_VALUE_HEADS
    trailing_length = REACH * NEARBY_TOKENS
    key_length = trailing_length + NEARBY_TOKENS
    score_scale = 1.0 / math.sqrt(HEAD_SIZE)
    positions = lax.iota(jnp.int32, PACKED_TOKENS)
    docs = doc_of(lengths, positions)
    filled_keys = jnp.concatenate([jnp.zeros((trailing_length, KEY_VALUE_HEADS * HEAD_SIZE), jnp.bfloat16), keys], 0)
    filled_values = jnp.concatenate([jnp.zeros((trailing_length, KEY_VALUE_HEADS * HEAD_SIZE), jnp.bfloat16), values], 0)
    padded_docs = jnp.concatenate([jnp.full((trailing_length,), -1, jnp.int32), docs], 0)

    def one_block(block_index):
        start_row = (block_index * NEARBY_TOKENS).astype(jnp.int32)
        query_matrix = lax.dynamic_slice_in_dim(query, start_row, NEARBY_TOKENS, 0).astype(jnp.float32)
        query_matrix = query_matrix.reshape(NEARBY_TOKENS, KEY_VALUE_HEADS, group_width, HEAD_SIZE)
        key_matrix = lax.dynamic_slice_in_dim(filled_keys, start_row, key_length, 0).astype(jnp.float32)
        key_matrix = key_matrix.reshape(key_length, KEY_VALUE_HEADS, HEAD_SIZE)
        value_matrix = lax.dynamic_slice_in_dim(filled_values, start_row, key_length, 0).astype(jnp.float32)
        value_matrix = value_matrix.reshape(key_length, KEY_VALUE_HEADS, HEAD_SIZE)
        query_docs = lax.dynamic_slice_in_dim(docs, start_row, NEARBY_TOKENS, 0)
        key_docs = lax.dynamic_slice_in_dim(padded_docs, start_row, key_length, 0)
        query_pos = start_row + lax.iota(jnp.int32, NEARBY_TOKENS)
        key_pos = start_row - trailing_length + lax.iota(jnp.int32, key_length)
        visible = (query_docs[:, None] == key_docs[None, :]) & (key_pos[None, :] <= query_pos[:, None])

        def one_head(operands):
            query_heads, key_heads, value_heads = operands
            scores = jnp.einsum('qgd,cd->gqc', query_heads, key_heads) * score_scale
            masked = jnp.where(visible[None], scores, -1e+30)
            top = lax.optimization_barrier(jnp.max(masked, axis=2))
            weights = jnp.where(visible[None], jnp.exp(masked - top[..., None]), 0.0)
            total = lax.optimization_barrier(jnp.sum(weights, axis=2))
            rounded = lax.optimization_barrier(weights.astype(jnp.bfloat16)).astype(jnp.float32)
            summed = jnp.einsum('gqc,cd->qgd', rounded, value_heads)
            return summed / jnp.transpose(total, (1, 0))[..., None]
        per_head = lax.map(one_head, (jnp.transpose(query_matrix, (1, 0, 2, 3)), jnp.transpose(key_matrix, (1, 0, 2)), jnp.transpose(value_matrix, (1, 0, 2))))
        return jnp.transpose(per_head, (1, 0, 2, 3)).reshape(NEARBY_TOKENS, QUERY_HEAD_COUNT * HEAD_SIZE).astype(jnp.bfloat16)
    blocks = lax.map(one_block, lax.iota(jnp.int32, PACKED_TOKENS // NEARBY_TOKENS))
    return blocks.reshape(PACKED_TOKENS, QUERY_HEAD_COUNT * HEAD_SIZE)
```

```python
import math

import jax
import jax.numpy as jnp
from jax import lax
from jax.experimental import pallas as pl
from jax.experimental.pallas import tpu as pltpu
from jax.sharding import PartitionSpec as P

D = 128
T = 128
C = 2 * T
KH = 4
GW = 8
W = KH * D
QW = W * GW
BLOCKS = 32
CHIPS = 4 * BLOCKS
NDOCS = 32
MASKED = -1e30
SCALE = 1.4426950408889634 / math.sqrt(D)
MESH = pl.DeviceIdType.MESH

OWN = 0
PREV = {0: 1, 3: 3, 1: 4, 2: 7}
OTHER = {0: 2, 3: 5, 1: 6, 2: 8}


def kernel(
    len_ref, q_ref, k_ref, v_ref, o_ref,
    qbuf, kbuf, vbuf, kfeat, qfeat, top, total, acc, obuf,
    local_sem, out_sem, own_sem, recv_sem, send0, send1, send2, send3, sendx,
    osend, orecv,
):
    head = lax.axis_index("head")
    b = lax.axis_index("outer") * 16 + lax.axis_index("inner")
    zh = head // 2
    c = head % 2

    def device(block, place, core):
        return {
            "head": place * 2 + core,
            "outer": block // 16,
            "inner": block % 16,
        }

    partner = device(b, zh, 1 - c)
    after = lambda core: device((b + 1) % BLOCKS, zh, core)
    before = lambda core: device((b + BLOCKS - 1) % BLOCKS, zh, core)
    beside = lambda dz, core: device(b, (zh + dz) % 4, core)

    def rows(core):
        return pl.ds(pl.multiple_of(core * T, T), T)

    def cols(core, width):
        return pl.ds(pl.multiple_of(core * width, width), width)

    @pl.when(b < 2)
    def _():
        def clear(i, carry):
            kbuf[i + 1] = jnp.zeros((C, W), jnp.bfloat16)
            vbuf[i + 1] = jnp.zeros((C, W), jnp.bfloat16)
            return carry

        lax.fori_loop(0, 8, clear, 0)

    local = [
        pltpu.make_async_copy(k_ref.at[:, cols(c, W)], kbuf.at[OWN, rows(c), :], local_sem.at[0]),
        pltpu.make_async_copy(v_ref.at[:, cols(c, W)], vbuf.at[OWN, rows(c), :], local_sem.at[1]),
        pltpu.make_async_copy(q_ref.at[:, cols(c, QW)], qbuf.at[rows(c), :], local_sem.at[2]),
    ]
    for copy in local:
        copy.start()

    barrier = pltpu.get_barrier_semaphore()
    greeted = [partner, after(0), after(1), before(0), before(1)]
    greeted += [beside(dz, core) for dz in (1, 2, 3) for core in (c, 1 - c)]
    for target in greeted:
        pl.semaphore_signal(barrier, inc=1, device_id=target, device_id_type=MESH)

    pl.semaphore_wait(barrier, len(greeted))

    def send(src, dst, send_sem, recv, target):
        return pltpu.make_async_remote_copy(
            src_ref=src, dst_ref=dst, send_sem=send_sem, recv_sem=recv,
            device_id=target, device_id_type=MESH,
        )

    bufs = (kbuf, vbuf)
    inputs = (k_ref, v_ref)

    first = []
    for i in range(2):
        core = (c + i) % 2
        for kv in range(2):
            first.append(
                send(
                    inputs[kv].at[:, cols(core, W)],
                    bufs[kv].at[PREV[0], rows(c), :],
                    send1.at[i, kv],
                    recv_sem.at[PREV[0], c, kv],
                    after(core),
                )
            )
    own = [
        send(
            inputs[kv].at[:, cols(1 - c, W)],
            bufs[kv].at[OWN, rows(c), :],
            send0.at[kv],
            own_sem.at[kv],
            partner,
        )
        for kv in range(2)
    ]
    own.append(
        send(q_ref.at[:, cols(1 - c, QW)], qbuf.at[rows(c), :], send0.at[2], own_sem.at[2], partner)
    )
    last = []
    for dz in (1, 2, 3):
        for i in range(2):
            core = (c + i) % 2
            for kv in range(2):
                last.append(
                    (
                        dz,
                        send(
                            inputs[kv].at[:, cols(core, W)],
                            bufs[kv].at[OTHER[4 - dz], rows(c), :],
                            sendx.at[dz - 1, i, kv],
                            recv_sem.at[OTHER[4 - dz], c, kv],
                            beside(dz, core),
                        ),
                    )
                )

    @pl.when(b < BLOCKS - 1)
    def _():
        for copy in first:
            copy.start()

    for copy in own:
        copy.start()

    for dz in (1, 2, 3):

        @pl.when((b == BLOCKS - 1) & (zh + dz < 4))
        def _():
            for place, copy in last:
                if place == dz:
                    copy.start()

    lane = lax.broadcasted_iota(jnp.int32, (1, 128), 1)
    begins = jnp.zeros((1, 128), jnp.int32)
    ends = jnp.zeros((1, 128), jnp.int32)
    end = jnp.int32(0)
    for j in range(NDOCS):
        begins = jnp.where(lane == j, end, begins)
        end = end + len_ref[j]
        ends = jnp.where(lane == j, end, ends)

    row_in_piece = lax.broadcasted_iota(jnp.int32, (C, 128), 0)

    def inside(chip):
        position = row_in_piece + (chip % CHIPS) * C
        return (position >= begins) & (position < ends)

    here = 4 * b + zh
    qfeat[...] = jnp.where(inside(here), 0.0, MASKED).astype(jnp.bfloat16)
    kfeat[OWN] = jnp.where(inside(here), 1.0, 0.0).astype(jnp.bfloat16)
    for r in range(4):
        chip = 4 * (b + BLOCKS - 1) + (zh + r) % 4
        kfeat[PREV[r]] = jnp.where(inside(chip), 1.0, 0.0).astype(jnp.bfloat16)
        chip = 4 * (b + BLOCKS - 2) + zh + r + 4 * ((zh + r) // 4)
        kfeat[OTHER[r]] = jnp.where(inside(chip), 1.0, 0.0).astype(jnp.bfloat16)

    ones = jnp.ones((C, D), jnp.bfloat16)

    def scores_of(slot, g):
        features = qfeat[...]
        queries = jnp.concatenate(
            [
                jnp.concatenate(
                    [qbuf[:, pl.ds(pl.multiple_of(g * GW * D, D) + j * D, D)], features], axis=1
                )
                for j in range(GW)
            ],
            axis=0,
        )
        keys = jnp.concatenate(
            [kbuf[slot, :, pl.ds(pl.multiple_of(g * D, D), D)], kfeat[slot]], axis=1
        )
        return lax.dot_general(
            queries, keys, (((1,), (1,)), ((), ())), preferred_element_type=jnp.float32
        )

    def summed(weights, slot, g):
        held = jnp.concatenate([vbuf[slot, :, pl.ds(pl.multiple_of(g * D, D), D)], ones], axis=1)
        return jnp.dot(weights.astype(jnp.bfloat16), held, preferred_element_type=jnp.float32)

    def attend_own(g, carry):
        scores = scores_of(OWN, g)
        key_at = lax.broadcasted_iota(jnp.int32, (GW * C, C), 1)
        query_at = lax.broadcasted_iota(jnp.int32, (GW * C, C), 0) & (C - 1)
        scores = jnp.where(key_at <= query_at, scores, MASKED)
        new_top = jnp.max(scores, axis=1, keepdims=True)
        both = summed(jnp.exp2((scores - new_top) * SCALE), OWN, g)
        top[g] = jnp.broadcast_to(new_top, (GW * C, D))
        acc[g] = both[:, :D]
        total[g] = both[:, D:]
        return carry

    def attend(slot, g):
        scores = scores_of(slot, g)
        old_top = top[g]
        new_top = jnp.maximum(old_top, jnp.max(scores, axis=1, keepdims=True))
        both = summed(jnp.exp2((scores - new_top[:, :1]) * SCALE), slot, g)
        shrink = jnp.exp2((old_top - new_top) * SCALE)
        top[g] = new_top
        acc[g] = acc[g] * shrink + both[:, :D]
        total[g] = total[g] * shrink + both[:, D:]

    def arrival(slot, sub, kv):
        part = bufs[kv].at[slot, rows(sub), :]
        return send(part, part, send0.at[0], recv_sem.at[slot, sub, kv], partner)

    def beside_send(slot, there, sub, kv, dz, index):
        return send(
            bufs[kv].at[slot, rows(sub), :],
            bufs[kv].at[there, rows(sub), :],
            send2.at[index, sub, kv],
            recv_sem.at[there, sub, kv],
            beside(dz, c),
        )

    def onward(r, sub, kv):
        forth = 1 - 2 * ((zh + r) // 4)
        return send(
            bufs[kv].at[PREV[r], rows(sub), :],
            bufs[kv].at[OTHER[r], rows(sub), :],
            send3.at[r, sub, kv],
            recv_sem.at[OTHER[r], sub, kv],
            device((b + BLOCKS + forth) % BLOCKS, zh, c),
        )

    def goes_onward(r):
        back = zh + r >= 4
        if r == 0:
            return (b > 0) & (b < BLOCKS - 1)
        return (b > 0) & (back | ((b < BLOCKS - 1) & (b != 15)))

    def start_onward(r, sub):
        @pl.when(goes_onward(r))
        def _():
            for kv in range(2):
                onward(r, sub, kv).start()

    def take_first(sub):
        @pl.when(b > 0)
        def _():
            for kv in range(2):
                arrival(PREV[0], sub, kv).wait_recv()
                beside_send(PREV[0], PREV[3], sub, kv, 1, 0).start()
                beside_send(PREV[0], PREV[1], sub, kv, 3, 1).start()

        start_onward(0, sub)

    def right_relay(kv):
        return send(
            bufs[kv].at[PREV[3], pl.ds(0, T), :],
            bufs[kv].at[PREV[2], pl.ds(0, T), :],
            send2.at[2, 0, kv],
            recv_sem.at[PREV[2], 0, kv],
            beside(1, c),
        )

    def left_relay(kv):
        return send(
            bufs[kv].at[PREV[1], pl.ds(T, T), :],
            bufs[kv].at[PREV[2], pl.ds(T, T), :],
            send2.at[2, 1, kv],
            recv_sem.at[PREV[2], 1, kv],
            beside(3, c),
        )

    def take_beside(sub):
        @pl.when(b > 0)
        def _():
            for kv in range(2):
                arrival(PREV[3], sub, kv).wait_recv()
                arrival(PREV[1], sub, kv).wait_recv()

            @pl.when(sub == 0)
            def _():
                for kv in range(2):
                    right_relay(kv).start()

            @pl.when(sub == 1)
            def _():
                for kv in range(2):
                    left_relay(kv).start()

        start_onward(3, sub)
        start_onward(1, sub)

    def take_relayed():
        @pl.when(b > 0)
        def _():
            for sub in range(2):
                for kv in range(2):
                    arrival(PREV[2], sub, kv).wait_recv()

        for sub in range(2):
            start_onward(2, sub)

    def across(dz, sub, kv):
        return send(
            bufs[kv].at[OTHER[0], rows(sub), :],
            bufs[kv].at[OTHER[4 - dz], rows(sub), :],
            sendx.at[dz - 1, sub, kv],
            recv_sem.at[OTHER[4 - dz], sub, kv],
            beside(dz, c),
        )

    def take_other(r):
        @pl.when((zh + r >= 4) | (b >= 2))
        def _():
            for sub in range(2):
                for kv in range(2):
                    arrival(OTHER[r], sub, kv).wait_recv()

        if r == 0:
            for dz in (1, 2, 3):

                @pl.when((b == 16) & (zh + dz >= 4))
                def _():
                    for sub in range(2):
                        for kv in range(2):
                            across(dz, sub, kv).start()

    for copy in local:
        copy.wait()
    for copy in own:
        copy.wait_recv()

    lax.fori_loop(0, KH, attend_own, 0)
    take_first(c)
    take_first(1 - c)

    def take_sixth():
        take_relayed()
        take_other(1)

    schedule = {
        (2, 0): lambda: take_other(0),
        (2, 2): lambda: take_beside(c),
        (3, 0): lambda: take_beside(1 - c),
        (5, 0): lambda: take_other(3),
        (6, 0): lambda: take_sixth(),
        (8, 0): lambda: take_other(2),
    }

    def step(t, carry):
        for (slot, g), action in schedule.items():
            pl.when(t == slot * KH + g)(action)
        attend(t // KH, t % KH)
        return carry

    lax.fori_loop(KH, 9 * KH, step, 0)

    outgoing = []
    for g in range(KH):
        outcome = (acc[g] / total[g]).astype(jnp.bfloat16)
        for j in range(GW):
            obuf[:, pl.ds((g * GW + j) * D, D)] = outcome[j * C : (j + 1) * C]
        part = pl.ds(g * GW * D, GW * D)
        place = pl.ds(pl.multiple_of(c * QW, QW) + g * GW * D, GW * D)
        kept = pltpu.make_async_copy(obuf.at[rows(c), part], o_ref.at[:, place], out_sem.at[g])
        given = send(
            obuf.at[rows(1 - c), part], o_ref.at[:, place], osend.at[g], orecv.at[g], partner
        )
        given.start()
        kept.start()
        outgoing.append((kept, given))

    for kept, given in outgoing:
        kept.wait()
        given.wait()
    for copy in own:
        copy.wait_send()

    @pl.when(b < BLOCKS - 1)
    def _():
        for copy in first:
            copy.wait_send()

    for dz in (1, 2, 3):

        @pl.when((b == BLOCKS - 1) & (zh + dz < 4))
        def _():
            for place, copy in last:
                if place == dz:
                    copy.wait_send()

        @pl.when((b == 16) & (zh + dz >= 4))
        def _():
            for sub in range(2):
                for kv in range(2):
                    across(dz, sub, kv).wait_send()

    @pl.when(b > 0)
    def _():
        for kv in range(2):
            for sub in range(2):
                beside_send(PREV[0], PREV[3], sub, kv, 1, 0).wait_send()
                beside_send(PREV[0], PREV[1], sub, kv, 3, 1).wait_send()
            right_relay(kv).wait_send()
            left_relay(kv).wait_send()

    for r in range(4):

        @pl.when(goes_onward(r))
        def _():
            for sub in range(2):
                for kv in range(2):
                    onward(r, sub, kv).wait_send()


def per_device(query, keys, values, lengths):
    any_space = pl.BlockSpec(memory_space=pl.ANY)
    dma = pltpu.SemaphoreType.DMA
    return pl.pallas_call(
        kernel,
        out_shape=jax.ShapeDtypeStruct(query.shape, jnp.bfloat16),
        in_specs=[pl.BlockSpec(memory_space=pltpu.SMEM), any_space, any_space, any_space],
        out_specs=any_space,
        scratch_shapes=[
            pltpu.VMEM((C, QW), jnp.bfloat16),
            pltpu.VMEM((9, C, W), jnp.bfloat16),
            pltpu.VMEM((9, C, W), jnp.bfloat16),
            pltpu.VMEM((9, C, 128), jnp.bfloat16),
            pltpu.VMEM((C, 128), jnp.bfloat16),
            pltpu.VMEM((KH, GW * C, D), jnp.float32),
            pltpu.VMEM((KH, GW * C, D), jnp.float32),
            pltpu.VMEM((KH, GW * C, D), jnp.float32),
            pltpu.VMEM((C, QW), jnp.bfloat16),
            dma((3,)),
            dma((KH,)),
            dma((3,)),
            dma((9, 2, 2)),
            dma((3,)),
            dma((2, 2)),
            dma((3, 2, 2)),
            dma((4, 2, 2)),
            dma((3, 2, 2)),
            dma((KH,)),
            dma((KH,)),
        ],
        compiler_params=pltpu.CompilerParams(
            collective_id=0, has_side_effects=True, vmem_limit_bytes=58 * 1024 * 1024
        ),
        name="attend_pack",
    )(lengths, query, keys, values)


def solution(mesh):
    placed = P(("outer", "inner", "head"), None)
    return jax.shard_map(
        per_device,
        mesh=mesh,
        in_specs=(placed, placed, placed, P()),
        out_specs=placed,
        check_vma=False,
    )
```
